8 devices in a mesh: dp: 2 (over z, y), tp: 4 (over x, core).
Axes of the slice: x: 2, y: 2, z: 1, core: 2. Of those that a mesh axis runs over, the one named last changes fastest.
Arguments:
- hidden: bfloat16 [2, 1024, 2048], P('dp', 'tp'), parts along dimension 0
- grad_out: bfloat16 [2, 1024, 2048], P('dp', 'tp'), parts along dimension 0
- ln1_gain: bfloat16 [2048], replicated
- ln1_bias: bfloat16 [2048], replicated
- w_qkv: bfloat16 [2048, 3, 32, 64], P(None, None, 'tp')
- b_qkv: bfloat16 [3, 32, 64], P(None, 'tp')
- w_out: bfloat16 [32, 64, 2048], P('tp')
- b_out: bfloat16 [2048], replicated
- ln2_gain: bfloat16 [2048], replicated
- ln2_bias: bfloat16 [2048], replicated
- w_up: bfloat16 [2048, 8192], P(None, 'tp')
- b_up: bfloat16 [8192], P('tp')
- w_down: bfloat16 [8192, 2048], P('tp')
- b_down: bfloat16 [2048], replicated
Outputs:
- output 1: bfloat16 [2, 1024, 2048], P('dp', 'tp'), parts along dimension 0
- output 2: bfloat16 [2, 1024, 2048], P('dp', 'tp'), parts along dimension 0
- output 3: float32 [4096], P('dp'), parts along dimension 0
- output 4: float32 [4096], P('dp'), parts along dimension 0
- output 5: float32 [4096, 3, 32, 64], P('dp', None, 'tp'), parts along dimension 0
- output 6: float32 [6, 32, 64], P('dp', 'tp'), parts along dimension 0
- output 7: float32 [64, 64, 2048], P(('dp', 'tp')), parts along dimension 0
- output 8: float32 [4096], P('dp'), parts along dimension 0
- output 9: float32 [4096], P('dp'), parts along dimension 0
- output 10: float32 [4096], P('dp'), parts along dimension 0
- output 11: float32 [4096, 8192], P('dp', 'tp'), parts along dimension 0
- output 12: float32 [16384], P(('dp', 'tp')), parts along dimension 0
- output 13: float32 [16384, 2048], P(('dp', 'tp')), parts along dimension 0
- output 14: float32 [4096], P('dp'), parts along dimension 0
There are 2 independent parts. The reference program is written for one: setup_inputs(seed, part) draws one part's arguments, and reference() takes and returns one part's arrays. A program takes and returns all parts, laid end to end along the dimension named above; an argument that names none is the same for every part.
All inputs are finite; a program needn't handle non-finite values.
Results may differ from the reference program's by a relative error of at most 0.0181765.
Values are sent between devices in bfloat16 or wider.
A program may use at most 1 GiB of HBM per device.

```python
import jax
import jax.numpy as jnp
from jax import lax

D_MODEL = 2048
HEADS = 32
HEAD_DIM = 64
FF_DIM = 8192
BATCH = 1
SEQ_LEN = 1024
LN_EPS = 1e-5


def draw_normal(key, shape, scale):
    return jax.random.normal(key, shape, jnp.float32) * scale


def setup_inputs(seed: int = 0, part: int = 0) -> dict:
    base_key = jax.random.key(seed)
    act_keys = jax.random.split(jax.random.fold_in(base_key, part), 2)
    weight_keys = jax.random.split(jax.random.fold_in(base_key, 100003), 12)
    d_scale = D_MODEL ** -0.5
    inputs = {
        "hidden": draw_normal(act_keys[0], (BATCH, SEQ_LEN, D_MODEL), 1.0),
        "grad_out": draw_normal(act_keys[1], (BATCH, SEQ_LEN, D_MODEL), 1.0),
        "ln1_gain": 1.0 + draw_normal(weight_keys[0], (D_MODEL,), 0.3),
        "ln1_bias": draw_normal(weight_keys[1], (D_MODEL,), 0.3),
        "w_qkv": draw_normal(weight_keys[2], (D_MODEL, 3, HEADS, HEAD_DIM), d_scale),
        "b_qkv": draw_normal(weight_keys[3], (3, HEADS, HEAD_DIM), 0.5),
        "w_out": draw_normal(weight_keys[4], (HEADS, HEAD_DIM, D_MODEL), d_scale),
        "b_out": draw_normal(weight_keys[5], (D_MODEL,), 0.3),
        "ln2_gain": 1.0 + draw_normal(weight_keys[6], (D_MODEL,), 0.3),
        "ln2_bias": draw_normal(weight_keys[7], (D_MODEL,), 0.3),
        "w_up": draw_normal(weight_keys[8], (D_MODEL, FF_DIM), d_scale),
        "b_up": draw_normal(weight_keys[9], (FF_DIM,), 0.3),
        "w_down": draw_normal(weight_keys[10], (FF_DIM, D_MODEL), FF_DIM ** -0.5),
        "b_down": draw_normal(weight_keys[11], (D_MODEL,), 0.3),
    }
    return {name: value.astype(jnp.bfloat16) for name, value in inputs.items()}


def as_bf16(value):
    return value.astype(jnp.bfloat16).astype(jnp.float32)


def layer_norm(value, gain, shift):
    centered = value - jnp.mean(value, axis=-1, keepdims=True)
    variance = jnp.mean(centered * centered, axis=-1, keepdims=True)
    return centered * lax.rsqrt(variance + LN_EPS) * gain + shift


def layer_forward(params, hidden):
    ln1_gain, ln1_bias, w_qkv, b_qkv, w_out, b_out, ln2_gain, ln2_bias, w_up, b_up, w_down, b_down = params
    normed1 = as_bf16(layer_norm(hidden, ln1_gain, ln1_bias))
    qkv_proj = as_bf16(jnp.einsum("bsd,dche->bsche", normed1, w_qkv) + b_qkv)
    scores = jnp.einsum("bqhe,bkhe->bhqk", qkv_proj[:, :, 0], qkv_proj[:, :, 1]) * (HEAD_DIM ** -0.5)
    positions = jnp.arange(SEQ_LEN)
    causal = positions[:, None] >= positions[None, :]
    attn_probs = as_bf16(jax.nn.softmax(jnp.where(causal, scores, -1e30), axis=-1))
    context = as_bf16(jnp.einsum("bhqk,bkhe->bqhe", attn_probs, qkv_proj[:, :, 2]))
    resid1 = as_bf16(hidden + jnp.einsum("bqhe,hed->bqd", context, w_out) + b_out)
    normed2 = as_bf16(layer_norm(resid1, ln2_gain, ln2_bias))
    pre_act = as_bf16(jnp.einsum("bsd,df->bsf", normed2, w_up) + b_up)
    gelu_out = as_bf16(jax.nn.gelu(pre_act, approximate=True))
    return as_bf16(resid1 + jnp.einsum("bsf,fd->bsd", gelu_out, w_down) + b_down)


def reference(hidden, grad_out, ln1_gain, ln1_bias, w_qkv, b_qkv, w_out, b_out, ln2_gain, ln2_bias, w_up, b_up, w_down, b_down):
    weights = (ln1_gain, ln1_bias, w_qkv, b_qkv, w_out, b_out, ln2_gain, ln2_bias, w_up, b_up, w_down, b_down)
    params = tuple(param.astype(jnp.float32) for param in weights)
    layer_out, pullback = jax.vjp(layer_forward, params, hidden.astype(jnp.float32))
    grad_params, grad_hidden = pullback(grad_out.astype(jnp.float32))
    return (layer_out.astype(jnp.bfloat16), grad_hidden.astype(jnp.bfloat16), grad_params[0], grad_params[1], grad_params[2], grad_params[3], grad_params[4], grad_params[5], grad_params[6], grad_params[7], grad_params[8], grad_params[9], grad_params[10], grad_params[11])
```

```python
import functools
import math

import jax
import jax.numpy as jnp
from jax import lax
from jax.experimental import pallas as pl
from jax.experimental.pallas import tpu as pltpu
from jax.sharding import PartitionSpec as P

LN_EPS = 1e-5
F32 = jnp.float32
BF16 = jnp.bfloat16
BLK = 256
NB = 4


def mm(a, b, ca, cb):
    return lax.dot_general(a, b, (((ca,), (cb,)), ((), ())), preferred_element_type=F32)


def places():
    me = lax.axis_index("tp")
    return [pl.ds(pl.multiple_of(jnp.bitwise_xor(me, c) * BLK, BLK), BLK) for c in range(NB)]


def causal_mask():
    rows = lax.broadcasted_iota(jnp.int32, (BLK, BLK), 0)
    cols = lax.broadcasted_iota(jnp.int32, (BLK, BLK), 1)
    return rows <= cols


def attn_fwd_kernel(scale, qkv_ref, o_ref, st_ref):
    at = places()
    q = [qkv_ref[0, 0, :, at[c]] for c in range(NB)]
    k = [qkv_ref[1, 0, :, at[c]] for c in range(NB)]
    v = [qkv_ref[2, 0, :, at[c]] for c in range(NB)]
    kt = jnp.concatenate(k, axis=1)
    vt = jnp.concatenate(v, axis=1)
    mask = causal_mask()
    for c in range(NB):
        n = (c + 1) * BLK
        s = mm(kt[:, :n], q[c], 0, 0)
        diag = jnp.where(mask, s[c * BLK:], -1e30)
        s = diag if c == 0 else jnp.concatenate([s[: c * BLK], diag], axis=0)
        m = jnp.max(s, axis=0, keepdims=True)
        e = jnp.exp2((s - m) * scale)
        r = 1.0 / jnp.sum(e, axis=0, keepdims=True)
        p = (e * r).astype(BF16)
        o_ref[0, :, at[c]] = mm(vt[:, :n], p, 1, 0).astype(BF16)
        st_ref[0, 0:1, at[c]] = m
        st_ref[0, 1:2, at[c]] = r


def attn_bwd_kernel(scale, attn_scale, qkv_ref, do_ref, st_ref, d_ref, p_ref, ds_ref):
    at = places()
    q = [qkv_ref[0, 0, :, at[c]] for c in range(NB)]
    k = [qkv_ref[1, 0, :, at[c]] for c in range(NB)]
    v = [qkv_ref[2, 0, :, at[c]] for c in range(NB)]
    do = [do_ref[0, :, at[c]] for c in range(NB)]
    kt = jnp.concatenate(k, axis=1)
    vt = jnp.concatenate(v, axis=1)
    qt = jnp.concatenate(q, axis=1)
    dot = jnp.concatenate(do, axis=1)
    mask = causal_mask()
    for c in range(NB):
        n = (c + 1) * BLK
        cols = pl.ds(c * BLK, BLK)
        m = st_ref[0, 0:1, at[c]]
        r = st_ref[0, 1:2, at[c]]
        s = mm(kt[:, :n], q[c], 0, 0)
        p = jnp.exp2((s - m) * scale) * r
        diag = jnp.where(mask, p[c * BLK:], 0.0)
        p = diag if c == 0 else jnp.concatenate([p[: c * BLK], diag], axis=0)
        p_ref[:n, cols] = p.astype(BF16)
        dp = mm(vt[:, :n], do[c], 0, 0).astype(BF16).astype(F32)
        row_dot = jnp.sum(dp * p, axis=0, keepdims=True)
        ds = (p * (dp - row_dot)).astype(BF16)
        ds_ref[:n, cols] = ds
        d_ref[0, 0, :, at[c]] = (mm(kt[:, :n], ds, 1, 0) * attn_scale).astype(BF16)
    for i in range(NB):
        rows = pl.ds(i * BLK, BLK)
        cols = pl.ds(i * BLK, (NB - i) * BLK)
        d_ref[1, 0, :, at[i]] = (mm(qt[:, i * BLK:], ds_ref[rows, cols], 1, 1) * attn_scale).astype(BF16)
        d_ref[2, 0, :, at[i]] = mm(dot[:, i * BLK:], p_ref[rows, cols], 1, 1).astype(BF16)


def attn_forward(qkv):
    _, heads, dim, seq = qkv.shape
    attn_scale = dim ** -0.5
    return pl.pallas_call(
        functools.partial(attn_fwd_kernel, attn_scale * math.log2(math.e)),
        grid=(heads,),
        in_specs=[pl.BlockSpec((3, 1, dim, seq), lambda h: (0, h, 0, 0))],
        out_specs=[pl.BlockSpec((1, dim, seq), lambda h: (h, 0, 0)), pl.BlockSpec((1, 2, seq), lambda h: (h, 0, 0))],
        out_shape=[jax.ShapeDtypeStruct((heads, dim, seq), BF16), jax.ShapeDtypeStruct((heads, 2, seq), F32)],
        compiler_params=pltpu.CompilerParams(vmem_limit_bytes=48 << 20),
        cost_estimate=pl.CostEstimate(flops=10 * 2**30, bytes_accessed=4 << 20, transcendentals=0),
        name="attn_fwd",
    )(qkv)


def attn_backward(qkv, grad_o, stats):
    _, heads, dim, seq = qkv.shape
    attn_scale = dim ** -0.5
    return pl.pallas_call(
        functools.partial(attn_bwd_kernel, attn_scale * math.log2(math.e), attn_scale),
        grid=(heads,),
        in_specs=[pl.BlockSpec((3, 1, dim, seq), lambda h: (0, h, 0, 0)), pl.BlockSpec((1, dim, seq), lambda h: (h, 0, 0)), pl.BlockSpec((1, 2, seq), lambda h: (h, 0, 0))],
        out_specs=pl.BlockSpec((3, 1, dim, seq), lambda h: (0, h, 0, 0)),
        out_shape=jax.ShapeDtypeStruct((3, heads, dim, seq), BF16),
        scratch_shapes=[pltpu.VMEM((seq, seq), BF16), pltpu.VMEM((seq, seq), BF16)],
        compiler_params=pltpu.CompilerParams(vmem_limit_bytes=48 << 20),
        cost_estimate=pl.CostEstimate(flops=22 * 2**30, bytes_accessed=8 << 20, transcendentals=0),
        name="attn_bwd",
    )(qkv, grad_o, stats)


def norm_stats(val32):
    centered = val32 - jnp.mean(val32, axis=-1, keepdims=True)
    inv_std = lax.rsqrt(jnp.mean(centered * centered, axis=-1, keepdims=True) + LN_EPS)
    return centered * inv_std, inv_std


def norm_forward(value, gain, shift):
    x_hat, inv_std = norm_stats(value.astype(F32))
    return (x_hat * gain.astype(F32) + shift.astype(F32)).astype(BF16), x_hat, inv_std


def norm_backward(grad32, x_hat, inv_std, gain):
    grad_gain = jnp.sum(grad32 * x_hat, axis=0)
    grad_shift = jnp.sum(grad32, axis=0)
    scaled = grad32 * gain.astype(F32)
    grad_input = inv_std * (scaled - jnp.mean(scaled, axis=-1, keepdims=True) - x_hat * jnp.mean(scaled * x_hat, axis=-1, keepdims=True))
    return grad_input, grad_gain, grad_shift


def gelu_tanh(value):
    return jax.nn.gelu(value, approximate=True)


def over_chip(value):
    return lax.ppermute(value, "tp", [(i, i ^ 1) for i in range(NB)])


def over_link(value):
    return lax.ppermute(value, "tp", [(i, i ^ 2) for i in range(NB)])


def after(value, *others):
    return lax.optimization_barrier((value,) + others)[0]


def link_gather(parts):
    far2 = [over_link(part) for part in parts]
    far3 = [over_chip(part) for part in far2]
    return far2, far3


def scatter_far(part):
    rows = part.shape[0] // 2
    halves = []
    for lo in (0, rows // 2):
        hi = lo + rows // 2
        other = over_chip(part[rows + lo: rows + hi])
        halves.append(over_link((part[lo:hi].astype(F32) + other.astype(F32)).astype(BF16)))
    return halves


def scatter_near(part):
    rows = part.shape[0] // 2
    other = over_chip(part[rows:])
    return part[:rows].astype(F32) + other.astype(F32)


def sum_over_group(value):
    value = value + over_chip(value)
    return value + over_link(value)


def solution(mesh):
    def device_step(hidden, grad_out, ln1_gain, ln1_bias, w_qkv, b_qkv, w_out, b_out, ln2_gain, ln2_bias, w_up, b_up, w_down, b_down):
        d_model, _, heads, dim = w_qkv.shape
        x = hidden[0]
        dy0 = grad_out[0]
        half = x.shape[0] // 2
        wt_qkv = jnp.transpose(w_qkv, (1, 2, 3, 0)).reshape(3 * heads * dim, d_model)
        bias_qkv = b_qkv.astype(F32).reshape(3 * heads * dim, 1)
        wo = w_out.reshape(heads * dim, d_model)

        h1_0, x_hat1, inv_std1 = norm_forward(x, ln1_gain, ln1_bias)
        h1_2, h1_3 = link_gather([h1_0[:half], h1_0[half:]])
        h1_near = jnp.concatenate([h1_0, over_chip(h1_0)], axis=0)
        h1_far = jnp.concatenate(h1_2 + h1_3, axis=0)
        dy_src = after(dy0, h1_2[0])
        dy_2, dy_3 = link_gather([dy_src[:half], dy_src[half:]])
        dy_near = jnp.concatenate([dy0, over_chip(dy_src)], axis=0)
        dy_far = jnp.concatenate(dy_2 + dy_3, axis=0)
        h1_all = jnp.concatenate([h1_near, h1_far], axis=0)

        qkv = (mm(wt_qkv, h1_all, 1, 1) + bias_qkv).astype(BF16).reshape(3, heads, dim, 4 * BLK)
        context, stats = attn_forward(qkv)
        ctx = context.reshape(heads * dim, 4 * BLK)

        attn_far = mm(ctx[:, 2 * BLK:], wo, 0, 0).astype(BF16)
        attn_near = mm(ctx[:, :2 * BLK], wo, 0, 0).astype(BF16)
        from_far = scatter_far(attn_far)
        from_near = scatter_near(attn_near)
        x1, h2_0, x_hat2, inv_std2 = [], [], [], []
        for i in range(2):
            rows = slice(i * half, (i + 1) * half)
            total = from_near[rows] + from_far[i].astype(F32)
            x1.append((x[rows].astype(F32) + total + b_out.astype(F32)).astype(BF16))
            normed, hat, inv = norm_forward(x1[i], ln2_gain, ln2_bias)
            h2_0.append(normed)
            x_hat2.append(hat)
            inv_std2.append(inv)
        h2_2, h2_3 = link_gather(h2_0)
        h2_own = jnp.concatenate(h2_0, axis=0)
        h2_near = jnp.concatenate([h2_own, over_chip(h2_own)], axis=0)
        h2_far = jnp.concatenate(h2_2 + h2_3, axis=0)

        def mlp(h2_half, dy_half):
            z = (mm(h2_half, w_up, 1, 0) + b_up.astype(F32)).astype(BF16)
            gelu_val, gelu_pull = jax.vjp(gelu_tanh, z.astype(F32))
            g = gelu_val.astype(BF16)
            dg = mm(dy_half, w_down, 1, 1).astype(BF16)
            dz = gelu_pull(dg.astype(F32))[0].astype(BF16)
            dh2 = mm(dz, w_up, 1, 1).astype(BF16)
            return g, dz, dh2

        g_far, dz_far, dh2_far = mlp(h2_far, dy_far)
        g_near, dz_near, dh2_near = mlp(h2_near, dy_near)
        dh2_from_far = scatter_far(dh2_far)
        dh2_from_near = scatter_near(dh2_near)
        dx1_0 = []
        ln2_sums = []
        for i in range(2):
            rows = slice(i * half, (i + 1) * half)
            total = (dh2_from_near[rows] + dh2_from_far[i].astype(F32)).astype(BF16).astype(F32)
            grad_ln, gain_sum, shift_sum = norm_backward(total, x_hat2[i], inv_std2[i], ln2_gain)
            ln2_sums.append((gain_sum, shift_sum))
            dx1_0.append((dy0[rows].astype(F32) + grad_ln).astype(BF16))
        dx1_2, dx1_3 = link_gather(dx1_0)
        dx1_own = jnp.concatenate(dx1_0, axis=0)
        dx1_near = jnp.concatenate([dx1_own, over_chip(dx1_own)], axis=0)
        dx1_far = jnp.concatenate(dx1_2 + dx1_3, axis=0)
        dx1_all = jnp.concatenate([dx1_near, dx1_far], axis=0)

        g_all = jnp.concatenate([g_near, g_far], axis=0)
        dz_all = jnp.concatenate([dz_near, dz_far], axis=0)
        h2_all = jnp.concatenate([h2_near, h2_far], axis=0)
        dy_all = jnp.concatenate([dy_near, dy_far], axis=0)
        grad_w_down = mm(g_all, dy_all, 0, 0)
        grad_w_up = mm(h2_all, dz_all, 0, 0)
        grad_b_up = jnp.sum(dz_all, axis=0, dtype=F32)

        y_far = after(mm(g_far, w_down, 1, 0).astype(BF16), dx1_2[0])
        y_near = mm(g_near, w_down, 1, 0).astype(BF16)
        y_from_far = scatter_far(y_far)
        y_from_near = scatter_near(y_near)
        y = []
        for i in range(2):
            rows = slice(i * half, (i + 1) * half)
            y.append((x1[i].astype(F32) + y_from_near[rows] + y_from_far[i].astype(F32) + b_down.astype(F32)).astype(BF16))
        layer_out = jnp.concatenate(y, axis=0)

        grad_ctx = mm(wo, dx1_all, 1, 1).astype(BF16)
        dqkv = attn_backward(qkv, grad_ctx.reshape(heads, dim, 4 * BLK), stats).reshape(3 * heads * dim, 4 * BLK)
        dh1_far = mm(dqkv[:, 2 * BLK:], wt_qkv, 0, 0).astype(BF16)
        dh1_near = mm(dqkv[:, :2 * BLK], wt_qkv, 0, 0).astype(BF16)
        dh1_from_far = scatter_far(dh1_far)
        dh1_from_near = scatter_near(dh1_near)
        grad_w_out = mm(ctx, dx1_all, 1, 0).reshape(heads, dim, d_model)
        grad_wt_qkv = mm(dqkv, h1_all, 1, 0)
        grad_w_qkv = jnp.transpose(grad_wt_qkv.reshape(3, heads, dim, d_model), (3, 0, 1, 2))
        grad_b_qkv = jnp.sum(dqkv, axis=1, dtype=F32).reshape(3, heads, dim)
        dh1 = (dh1_from_near + jnp.concatenate(dh1_from_far, axis=0).astype(F32)).astype(BF16).astype(F32)
        grad_ln1, gain1_sum, shift1_sum = norm_backward(dh1, x_hat1, inv_std1, ln1_gain)
        grad_hidden = (dx1_own.astype(F32) + grad_ln1).astype(BF16)

        early = sum_over_group(jnp.stack([
            jnp.sum(dx1_own, axis=0, dtype=F32),
            ln2_sums[0][0] + ln2_sums[1][0],
            ln2_sums[0][1] + ln2_sums[1][1],
            jnp.sum(dy0, axis=0, dtype=F32),
        ]))
        late = sum_over_group(jnp.stack([gain1_sum, shift1_sum]))
        return (layer_out[None], grad_hidden[None], late[0], late[1], grad_w_qkv, grad_b_qkv, grad_w_out, early[0], early[1], early[2], grad_w_up, grad_b_up, grad_w_down, early[3])

    act_spec = P("dp", "tp", None)
    vec_spec = P(None)
    group_vec = P("dp")
    in_specs = (act_spec, act_spec, vec_spec, vec_spec, P(None, None, "tp", None), P(None, "tp", None), P("tp", None, None), vec_spec, vec_spec, vec_spec, P(None, "tp"), P("tp"), P("tp", None), vec_spec)
    out_specs = (act_spec, act_spec, group_vec, group_vec, P("dp", None, "tp", None), P("dp", "tp", None), P(("dp", "tp"), None, None), group_vec, group_vec, group_vec, P("dp", "tp"), P(("dp", "tp")), P(("dp", "tp"), None), group_vec)
    return jax.shard_map(device_step, mesh=mesh, in_specs=in_specs, out_specs=out_specs, check_vma=False)
```

```python
import functools
import math

import jax
import jax.numpy as jnp
from jax import lax
from jax.experimental import pallas as pl
from jax.experimental.pallas import tpu as pltpu
from jax.sharding import PartitionSpec as P

LN_EPS = 1e-5
F32 = jnp.float32
BF16 = jnp.bfloat16
BLK = 256
NB = 4
GELU_C = math.sqrt(2.0 / math.pi)
GELU_A = 0.044715


def mm(a, b, ca, cb):
    return lax.dot_general(a, b, (((ca,), (cb,)), ((), ())), preferred_element_type=F32)


def sds(shape, dtype=BF16):
    return jax.ShapeDtypeStruct(shape, dtype)


def whole(shape):
    return pl.BlockSpec(shape, lambda *_: (0,) * len(shape))


def call(body, name, grid, ins, in_specs, outs, out_specs, flops=0, scratch=()):
    moved = sum(math.prod(a.shape) * a.dtype.itemsize for a in list(ins) + list(outs))
    return pl.pallas_call(
        body,
        grid=grid,
        in_specs=in_specs,
        out_specs=out_specs,
        out_shape=outs,
        scratch_shapes=list(scratch),
        compiler_params=pltpu.CompilerParams(vmem_limit_bytes=56 << 20),
        cost_estimate=pl.CostEstimate(flops=int(flops) + moved * 100, bytes_accessed=moved, transcendentals=0),
        name=name,
    )(*ins)


def causal_mask():
    rows = lax.broadcasted_iota(jnp.int32, (BLK, BLK), 0)
    cols = lax.broadcasted_iota(jnp.int32, (BLK, BLK), 1)
    return rows <= cols


def lanes(block):
    return pl.ds(pl.multiple_of(block * BLK, BLK), BLK)


def in_order(dst, near, far, index):
    me = lax.axis_index("tp")
    for j in range(NB):
        src = near if j < 2 else far
        dst[:, lanes(jnp.bitwise_xor(me, j))] = src[index + (slice(None), slice((j % 2) * BLK, (j % 2 + 1) * BLK))]


def out_of_order(src, near, far, index):
    me = lax.axis_index("tp")
    for j in range(NB):
        dst = near if j < 2 else far
        dst[index + (slice(None), slice((j % 2) * BLK, (j % 2 + 1) * BLK))] = src[:, lanes(jnp.bitwise_xor(me, j))]


def attn_fwd_kernel(scale, near_ref, far_ref, on_ref, of_ref, st_ref, q_s, k_s, v_s, o_s):
    for part, dst in enumerate((q_s, k_s, v_s)):
        in_order(dst, near_ref, far_ref, (part, 0))
    kt = k_s[...].T
    vt = v_s[...]
    mask = causal_mask()
    for c in range(NB):
        cols = slice(c * BLK, (c + 1) * BLK)
        n = (c + 1) * BLK
        q = q_s[:, cols]
        s = [mm(kt[i * BLK:(i + 1) * BLK], q, 1, 0) for i in range(c + 1)]
        s[c] = jnp.where(mask, s[c], -1e30)
        m = functools.reduce(jnp.maximum, [jnp.max(t, axis=0, keepdims=True) for t in s])
        e = [jnp.exp2((t - m) * scale) for t in s]
        r = 1.0 / functools.reduce(jnp.add, [jnp.sum(t, axis=0, keepdims=True) for t in e])
        p = jnp.concatenate([(t * r).astype(BF16) for t in e], axis=0)
        o_s[:, cols] = mm(vt[:, :n], p, 1, 0).astype(BF16)
        st_ref[0, 0:1, cols] = m
        st_ref[0, 1:2, cols] = r
    out_of_order(o_s, on_ref, of_ref, (0,))


def attn_bwd_kernel(scale, attn_scale, near_ref, far_ref, don_ref, dof_ref, st_ref, dn_ref, df_ref, q_s, k_s, v_s, do_s, d_s, p_ref, ds_ref):
    for part, dst in enumerate((q_s, k_s, v_s)):
        in_order(dst, near_ref, far_ref, (part, 0))
    in_order(do_s, don_ref, dof_ref, (0,))
    kt = k_s[...].T
    vt = v_s[...].T
    mask = causal_mask()
    for c in range(NB):
        cols = slice(c * BLK, (c + 1) * BLK)
        n = (c + 1) * BLK
        m = st_ref[0, 0:1, cols]
        r = st_ref[0, 1:2, cols]
        s = mm(kt[:n], q_s[:, cols], 1, 0)
        p = jnp.exp2((s - m) * scale) * r
        diag = jnp.where(mask, p[c * BLK:], 0.0)
        p = diag if c == 0 else jnp.concatenate([p[: c * BLK], diag], axis=0)
        p_ref[:n, cols] = p.astype(BF16)
        dp = mm(vt[:n], do_s[:, cols], 1, 0).astype(BF16).astype(F32)
        row_dot = jnp.sum(dp * p, axis=0, keepdims=True)
        ds = (p * (dp - row_dot)).astype(BF16)
        ds_ref[:n, cols] = ds
        d_s[0, :, cols] = (mm(k_s[:, :n], ds, 1, 0) * attn_scale).astype(BF16)
    for i in range(NB):
        rows = slice(i * BLK, (i + 1) * BLK)
        d_s[1, :, rows] = (mm(q_s[:, i * BLK:], ds_ref[rows, i * BLK:], 1, 1) * attn_scale).astype(BF16)
        d_s[2, :, rows] = mm(do_s[:, i * BLK:], p_ref[rows, i * BLK:], 1, 1).astype(BF16)
    for part in range(3):
        out_of_order(d_s.at[part], dn_ref, df_ref, (part, 0))


def attn_forward(near, far):
    _, heads, dim, half = near.shape
    attn_scale = dim ** -0.5
    qkv_spec = pl.BlockSpec((3, 1, dim, half), lambda h: (0, h, 0, 0))
    o_spec = pl.BlockSpec((1, dim, half), lambda h: (h, 0, 0))
    vm = pltpu.VMEM((dim, 2 * half), BF16)
    return call(
        functools.partial(attn_fwd_kernel, attn_scale * math.log2(math.e)), "attn_fwd", (heads,),
        [near, far], [qkv_spec, qkv_spec],
        [sds((heads, dim, half)), sds((heads, dim, half)), sds((heads, 2, 2 * half), F32)],
        [o_spec, o_spec, pl.BlockSpec((1, 2, 2 * half), lambda h: (h, 0, 0))],
        10e9, [vm] * 4)


def attn_backward(near, far, do_near, do_far, stats):
    _, heads, dim, half = near.shape
    attn_scale = dim ** -0.5
    qkv_spec = pl.BlockSpec((3, 1, dim, half), lambda h: (0, h, 0, 0))
    o_spec = pl.BlockSpec((1, dim, half), lambda h: (h, 0, 0))
    vm = pltpu.VMEM((dim, 2 * half), BF16)
    big = pltpu.VMEM((2 * half, 2 * half), BF16)
    return call(
        functools.partial(attn_bwd_kernel, attn_scale * math.log2(math.e), attn_scale), "attn_bwd", (heads,),
        [near, far, do_near, do_far, stats],
        [qkv_spec, qkv_spec, o_spec, o_spec, pl.BlockSpec((1, 2, 2 * half), lambda h: (h, 0, 0))],
        [sds(near.shape), sds(far.shape)], [qkv_spec, qkv_spec],
        22e9, [vm] * 4 + [pltpu.VMEM((3, dim, 2 * half), BF16), big, big])


def lay(dst, pieces):
    row = 0
    for piece in pieces:
        n = piece.shape[0]
        dst[row:row + n] = piece[...]
        row += n


def act_weight(pieces, w, name, transposed, out_rows=None, keep=False, step=512):
    rows = sum(p.shape[0] for p in pieces)
    inner = pieces[0].shape[1]
    n = w.shape[0] if transposed else w.shape[1]
    out_rows = out_rows or rows
    n_out = rows // out_rows
    n_in = len(pieces)

    def body(*refs):
        ins, w_ref, outs, a_ref = refs[:n_in], refs[n_in], refs[n_in + 1:n_in + 1 + n_out], refs[n_in + 1 + n_out]

        @pl.when(pl.program_id(0) == 0)
        def _():
            lay(a_ref, ins)

        t = mm(a_ref[...], w_ref[...], 1, 1 if transposed else 0).astype(BF16)
        for i, o in enumerate(outs):
            o[...] = t[i * out_rows:(i + 1) * out_rows]

    w_spec = pl.BlockSpec((step, inner), lambda i: (i, 0)) if transposed else pl.BlockSpec((inner, step), lambda i: (0, i))
    outs = [sds((out_rows, n))] * n_out
    out_specs = [pl.BlockSpec((out_rows, step), lambda i: (0, i))] * n_out
    scratch = [pltpu.VMEM((rows, inner), BF16)]
    if keep:
        outs, out_specs, scratch = outs + [sds((rows, inner))], out_specs + [whole((rows, inner))], []
    return call(body, name, (n // step,), list(pieces) + [w], [whole(p.shape) for p in pieces] + [w_spec], outs, out_specs, 2.0 * rows * inner * n, scratch)


def weight_act(w, pieces, name, bias=None, step=512):
    rows = sum(p.shape[0] for p in pieces)
    m, inner = w.shape
    n_in = len(pieces)
    has_bias = bias is not None

    def body(*refs):
        ins, w_ref = refs[:n_in], refs[n_in]
        o_ref, a_ref = refs[-2:]

        @pl.when(pl.program_id(0) == 0)
        def _():
            lay(a_ref, ins)

        t = mm(w_ref[...], a_ref[...], 1, 1)
        if has_bias:
            t = t + refs[n_in + 1][...]
        o_ref[...] = t.astype(BF16)

    ins = list(pieces) + [w] + ([bias] if has_bias else [])
    specs = [whole(p.shape) for p in pieces] + [pl.BlockSpec((step, inner), lambda i: (i, 0))]
    specs += [pl.BlockSpec((step, 1), lambda i: (i, 0))] if has_bias else []
    return call(body, name, (m // step,), ins, specs, [sds((m, rows)), sds((rows, inner))],
                [pl.BlockSpec((step, rows), lambda i: (i, 0)), whole((rows, inner))], 2.0 * rows * inner * m)


def feat_weight(a, w, name, out_rows, step=512):
    inner, rows = a.shape
    n = w.shape[1]
    n_out = rows // out_rows

    def body(a_ref, w_ref, *refs):
        outs, t_ref = refs[:n_out], refs[n_out]

        @pl.when(pl.program_id(0) == 0)
        def _():
            t_ref[...] = a_ref[...].T

        t = mm(t_ref[...], w_ref[...], 1, 0).astype(BF16)
        for i, o in enumerate(outs):
            o[...] = t[i * out_rows:(i + 1) * out_rows]

    return call(body, name, (n // step,), [a, w], [whole(a.shape), pl.BlockSpec((inner, step), lambda i: (0, i))],
                [sds((out_rows, n))] * n_out, [pl.BlockSpec((out_rows, step), lambda i: (0, i))] * n_out, 2.0 * rows * inner * n,
                [pltpu.VMEM((rows, inner), BF16)])


def feat_act(a, b, name, step):
    m, n = a[0].shape[0], b[0].shape[1]
    k = len(a)

    def body(*refs):
        total = mm(refs[0][...], refs[k][...], 1, 0)
        for i in range(1, k):
            total = total + mm(refs[i][...], refs[k + i][...], 1, 0)
        refs[-1][...] = total

    return call(body, name, (m // step,), list(a) + list(b), [pl.BlockSpec((step, t.shape[1]), lambda i: (i, 0)) for t in a] + [whole(t.shape) for t in b],
                [sds((m, n), F32)], [pl.BlockSpec((step, n), lambda i: (i, 0))], 2.0 * m * n * sum(t.shape[0] for t in b))[0]


def act_act(a, b, slices, name, step=256):
    m, n = a[0].shape[1], b[0].shape[1]
    ka, kb = len(a), len(b)

    def body(*refs):
        at = jnp.concatenate([refs[i][lo:hi] for i, lo, hi in slices], axis=0)
        total, row = None, 0
        for i in range(kb):
            r = refs[ka + i]
            t = mm(at[row:row + r.shape[0]], r[...], 0, 0)
            row += r.shape[0]
            total = t if total is None else total + t
        refs[-1][...] = total

    return call(body, name, (m // step,), list(a) + list(b), [pl.BlockSpec((t.shape[0], step), lambda i: (0, i)) for t in a] + [whole(t.shape) for t in b],
                [sds((m, n), F32)], [pl.BlockSpec((step, n), lambda i: (i, 0))], 2.0 * m * n * sum(t.shape[0] for t in b))[0]


def mlp(h2, dg, dg_blocks, w_up, b_up, name, out_rows, step=512, sub=256):
    rows = sum(p.shape[0] for p in h2)
    d, f = w_up.shape
    n_out = rows // out_rows
    n_in = len(h2)
    n_dg = len(dg_blocks)
    dg_rows = rows // n_dg

    def body(*refs):
        ins, dgs = refs[:n_in], refs[n_in:n_in + n_dg]
        w_ref, b_ref = refs[n_in + n_dg:n_in + n_dg + 2]
        outs = refs[n_in + n_dg + 2:]
        dh_refs, g_ref, dz_ref, db_ref, a_ref, acc_ref = outs[:n_out], outs[n_out], outs[n_out + 1], outs[n_out + 2], outs[n_out + 3], outs[n_out + 4]
        i = pl.program_id(0)

        @pl.when(i == 0)
        def _():
            lay(a_ref, ins)
            acc_ref[...] = jnp.zeros_like(acc_ref)

        for j in range(step // sub):
            cols = slice(j * sub, (j + 1) * sub)
            z = (mm(a_ref[...], w_ref[:, cols], 1, 0) + b_ref[:, cols].astype(F32)).astype(BF16).astype(F32)
            z2 = z * z
            t = jnp.tanh(z * (GELU_C + GELU_C * GELU_A * z2))
            cdf = 0.5 * (1.0 + t)
            slope = cdf + ((cdf * (1.0 - t)) * z) * (GELU_C + 3.0 * GELU_C * GELU_A * z2)
            g_ref[:, cols] = (z * cdf).astype(BF16)
            grad = jnp.concatenate([r[:, cols] for r in dgs], axis=0).astype(F32) if n_dg > 1 else dgs[0][:, cols].astype(F32)
            dz = (grad * slope).astype(BF16)
            dz_ref[:, cols] = dz
            db_ref[:, cols] = jnp.sum(dz.astype(F32), axis=0, keepdims=True)
        acc_ref[...] += mm(dz_ref[...], w_ref[...], 1, 1)

        @pl.when(i == pl.num_programs(0) - 1)
        def _():
            for k, o in enumerate(dh_refs):
                o[...] = acc_ref[k * out_rows:(k + 1) * out_rows].astype(BF16)

    def dg_spec(block):
        return pl.BlockSpec((dg_rows, step), lambda i: (block, i))

    ins = list(h2) + [dg] * n_dg + [w_up, b_up.reshape(1, f)]
    specs = [whole(p.shape) for p in h2] + [dg_spec(b) for b in dg_blocks] + [pl.BlockSpec((d, step), lambda i: (0, i)), pl.BlockSpec((1, step), lambda i: (0, i))]
    tile = pl.BlockSpec((rows, step), lambda i: (0, i))
    outs = [sds((out_rows, d))] * n_out + [sds((rows, f)), sds((rows, f)), sds((1, f), F32), sds((rows, d))]
    out_specs = [whole((out_rows, d))] * n_out + [tile, tile, pl.BlockSpec((1, step), lambda i: (0, i)), whole((rows, d))]
    res = call(body, name, (f // step,), ins, specs, outs, out_specs, 4.0 * rows * d * f, [pltpu.VMEM((rows, d), F32)])
    return list(res[:n_out]), res[n_out], res[n_out + 1], res[n_out + 2], res[n_out + 3]


def norm_stats(val32):
    centered = val32 - jnp.mean(val32, axis=-1, keepdims=True)
    inv_std = lax.rsqrt(jnp.mean(centered * centered, axis=-1, keepdims=True) + LN_EPS)
    return centered * inv_std, inv_std


def row_vec(v):
    return v.reshape(1, v.shape[0])


ROWS = 64


def row_spec(d, first=0):
    return pl.BlockSpec((ROWS, d), lambda i: (i + first, 0))


def norm_first(x, gain, shift, chunk, rows):
    d = x.shape[1]

    def body(x_ref, g_ref, s_ref, o_ref):
        x_hat, _ = norm_stats(x_ref[...].astype(F32))
        o_ref[...] = (x_hat * g_ref[...].astype(F32) + s_ref[...].astype(F32)).astype(BF16)

    return call(body, "norm1", (rows // ROWS,), [x, row_vec(gain), row_vec(shift)], [row_spec(d, chunk * rows // ROWS), whole((1, d)), whole((1, d))],
                [sds((rows, d))], [row_spec(d)])[0]


def norm_second(x, parts, bias, gain, shift, chunk, rows):
    d = x.shape[1]

    def body(x_ref, p0, p1, p2, b_ref, g_ref, s_ref, x1_ref, o_ref):
        total = p0[...].astype(F32) + p1[...].astype(F32) + p2[...].astype(F32)
        x1 = (x_ref[...].astype(F32) + total + b_ref[...].astype(F32)).astype(BF16)
        x1_ref[...] = x1
        x_hat, _ = norm_stats(x1.astype(F32))
        o_ref[...] = (x_hat * g_ref[...].astype(F32) + s_ref[...].astype(F32)).astype(BF16)

    vecs = [row_vec(bias), row_vec(gain), row_vec(shift)]
    return call(body, "norm2", (rows // ROWS,), [x] + parts + vecs, [row_spec(d, chunk * rows // ROWS)] + [row_spec(d)] * 3 + [whole((1, d))] * 3,
                [sds((rows, d))] * 2, [row_spec(d)] * 2)


def norm_back(parts, value, value_at, other, other_at, gain, rows, name):
    d = gain.shape[0]

    def body(p0, p1, p2, v_ref, y_ref, g_ref, o_ref, s_ref):
        grad = (p0[...].astype(F32) + p1[...].astype(F32) + p2[...].astype(F32)).astype(BF16).astype(F32)
        x_hat, inv_std = norm_stats(v_ref[...].astype(F32))
        scaled = grad * g_ref[...].astype(F32)
        back = inv_std * (scaled - jnp.mean(scaled, axis=-1, keepdims=True) - x_hat * jnp.mean(scaled * x_hat, axis=-1, keepdims=True))
        y = y_ref[...].astype(F32)
        out = (y + back).astype(BF16)
        o_ref[...] = out
        sums = [jnp.sum(t, axis=0, keepdims=True) for t in (grad * x_hat, grad, out.astype(F32), y)]
        first = pl.program_id(0) == 0
        for k, t in enumerate(sums):
            s_ref[k:k + 1] = jnp.where(first, t, s_ref[k:k + 1] + t)

    return call(body, name, (rows // ROWS,), parts + [value, other, row_vec(gain)],
                [row_spec(d)] * 3 + [row_spec(d, value_at * rows // ROWS), row_spec(d, other_at * rows // ROWS), whole((1, d))],
                [sds((rows, d)), sds((4, d), F32)], [row_spec(d), whole((4, d))])


def over_chip(value):
    return lax.ppermute(value, "tp", [(i, i ^ 1) for i in range(NB)])


def over_link(value):
    return lax.ppermute(value, "tp", [(i, i ^ 2) for i in range(NB)])


def after(value, *others):
    return lax.optimization_barrier((value,) + others)[0]


def add2(a, b):
    return (a.astype(F32) + b.astype(F32)).astype(BF16)


def sum_over_group(value):
    value = value + over_chip(value)
    return value + over_link(value)


def solution(mesh):
    def device_step(hidden, grad_out, ln1_gain, ln1_bias, w_qkv, b_qkv, w_out, b_out, ln2_gain, ln2_bias, w_up, b_up, w_down, b_down):
        d_model, _, heads, dim = w_qkv.shape
        x = hidden[0]
        dy_0 = grad_out[0]
        half = x.shape[0] // 2
        feats = heads * dim
        wt_qkv = jnp.transpose(w_qkv, (1, 2, 3, 0)).reshape(3 * feats, d_model)
        bias_qkv = b_qkv.astype(F32).reshape(3 * feats, 1)
        wo = w_out.reshape(feats, d_model)

        h1_0 = [norm_first(x, ln1_gain, ln1_bias, i, half) for i in range(2)]
        h1_2 = [over_link(t) for t in h1_0]
        h1_1 = [over_chip(t) for t in h1_0]
        dy_1 = over_chip(dy_0)
        dg_near, dy_near = act_weight([dy_0, dy_1], w_down, "dg", True, keep=True)
        qkv_near, h1_near = weight_act(wt_qkv, [h1_0[0], h1_0[1], after(h1_1[0], dg_near), h1_1[1]], "qkv", bias_qkv)
        h1_3 = [over_chip(t) for t in h1_2]
        dy_2 = over_link(after(dy_0, h1_2[0]))
        dy_3 = over_chip(dy_2)
        qkv_far, h1_far = weight_act(wt_qkv, [after(h1_2[0], qkv_near), h1_2[1], h1_3[0], h1_3[1]], "qkv", bias_qkv)
        shape = (3, heads, dim, 2 * BLK)
        qkv_near, qkv_far = qkv_near.reshape(shape), qkv_far.reshape(shape)
        ctx_near, ctx_far, stats = attn_forward(qkv_near, qkv_far)
        ctx_near, ctx_far = ctx_near.reshape(feats, 2 * BLK), ctx_far.reshape(feats, 2 * BLK)

        pf = feat_weight(ctx_far, wo, "out_proj", half)
        pn = feat_weight(after(ctx_near, pf[0]), wo, "out_proj", half)
        pf3 = [over_chip(t) for t in pf[2:]]
        pn1 = [over_chip(t) for t in pn[2:]]
        sent = [add2(pf[i], after(pf3[i], pn[0])) for i in range(2)]
        attn_x = [over_link(t) for t in sent]
        dg_far, dy_far = act_weight([after(dy_2, sent[1]), dy_3], w_down, "dg", True, keep=True)
        x1, h2_0, h2_1, h2_2, h2_3 = [], [], [], [], []
        for i in range(2):
            a, b = norm_second(x, [pn[i], pn1[i], after(attn_x[i], dg_far)], b_out, ln2_gain, ln2_bias, i, half)
            x1.append(a)
            h2_0.append(b)
            h2_2.append(over_link(b))
            h2_1.append(over_chip(b))
        h2_3 = [over_chip(t) for t in h2_2]

        dn, g_near, dz_near, db_near, h2_near = mlp([h2_0[0], h2_0[1], h2_1[0], h2_1[1]], dg_near, (0,), w_up, b_up, "mlp_near", half)
        dn1 = [over_chip(t) for t in dn[2:]]
        dfa, g_fa, dz_fa, db_fa, h2_fa = mlp([after(h2_2[0], dz_near), h2_3[0]], dg_far, (0, 2), w_up, b_up, "mlp_far", half)
        fa3 = over_chip(dfa[1])
        y_near = act_weight([after(g_near, dz_fa)], w_down, "y", False, half)
        sent_a = add2(dfa[0], after(fa3, y_near[0]))
        dh2_x = [over_link(sent_a)]
        dfb, g_fb, dz_fb, db_fb, h2_fb = mlp([after(h2_2[1], sent_a), h2_3[1]], dg_far, (1, 3), w_up, b_up, "mlp_far", half)
        fb3 = over_chip(dfb[1])
        y_far = act_weight([after(g_fa, dz_fb), g_fb], w_down, "y", False, half)
        sent_b = add2(dfb[0], after(fb3, y_far[0]))
        dh2_x.append(over_link(sent_b))
        grad_b_up = (db_near + db_fa + db_fb)[0]
        grad_w_down = act_act([after(g_near, sent_b), g_fa, g_fb], [dy_near, dy_far], [(0, 0, 512), (1, 0, 128), (2, 0, 128), (1, 128, 256), (2, 128, 256)], "dw_down")
        dx1_0, dx1_1, dx1_2, sums2 = [], [], [], []
        cover = [y_far[0], grad_w_down]
        for i in range(2):
            a, b = norm_back([dn[i], dn1[i], after(dh2_x[i], cover[i])], x1[i], 0, dy_0, i, ln2_gain, half, "norm2_back")
            dx1_0.append(a)
            sums2.append(b)
            dx1_2.append(over_link(a))
            dx1_1.append(over_chip(a))
        dx1_3 = [over_chip(t) for t in dx1_2]
        grad_w_up = act_act([after(h2_near, dx1_0[1]), h2_fa, h2_fb], [dz_near, dz_fa, dz_fb], [(0, 0, 512), (1, 0, 256), (2, 0, 256)], "dw_up")

        yf3 = [over_chip(y_far[1]), over_chip(y_far[3])]
        yn1 = [over_chip(t) for t in y_near[2:]]
        y_x = [over_link(add2(after(y_far[2 * i], dx1_2[0]), yf3[i])) for i in range(2)]

        do_near, dx1_near = weight_act(wo, [after(dx1_0[0], grad_w_up), dx1_0[1], dx1_1[0], dx1_1[1]], "d_ctx")
        do_far, dx1_far = weight_act(wo, [after(dx1_2[0], do_near), dx1_2[1], dx1_3[0], dx1_3[1]], "d_ctx")
        d_near, d_far = attn_backward(qkv_near, qkv_far, do_near.reshape(heads, dim, 2 * BLK), do_far.reshape(heads, dim, 2 * BLK), stats)
        d_near, d_far = d_near.reshape(3 * feats, 2 * BLK), d_far.reshape(3 * feats, 2 * BLK)
        hf = feat_weight(d_far, wt_qkv, "dh1", half)
        hf3 = [over_chip(t) for t in hf[2:]]
        hn = feat_weight(after(d_near, hf[0]), wt_qkv, "dh1", half)
        hn1 = [over_chip(t) for t in hn[2:]]
        sent = [add2(hf[i], after(hf3[i], hn[0])) for i in range(2)]
        dh1_x = [over_link(t) for t in sent]
        grad_wt_qkv = feat_act([after(d_near, sent[1]), d_far], [h1_near, h1_far], "dw_qkv", 256)
        grad_w_out = feat_act([after(ctx_near, grad_wt_qkv), ctx_far], [dx1_near, dx1_far], "dw_out", 256)
        grad_b_qkv = (jnp.sum(d_near, axis=1, dtype=F32) + jnp.sum(d_far, axis=1, dtype=F32)).reshape(3, heads, dim)
        y = []
        for i in range(2):
            total = yn1[i].astype(F32) + y_near[i].astype(F32) + after(y_x[i], grad_w_out).astype(F32)
            y.append((x1[i].astype(F32) + total + b_down.astype(F32)).astype(BF16))
        layer_out = jnp.concatenate(y, axis=0)
        early = sum_over_group(after(sums2[0] + sums2[1], sent[1]))
        dx, sums1 = [], []
        for i in range(2):
            a, b = norm_back([hn[i], hn1[i], after(dh1_x[i], grad_w_out)], x, i, dx1_0[i], 0, ln1_gain, half, "norm1_back")
            dx.append(a)
            sums1.append(b)
        grad_hidden = jnp.concatenate(dx, axis=0)
        late = sum_over_group((sums1[0] + sums1[1])[:2])
        grad_w_qkv = jnp.transpose(grad_wt_qkv.reshape(3, heads, dim, d_model), (3, 0, 1, 2))
        return (layer_out[None], grad_hidden[None], late[0], late[1], grad_w_qkv, grad_b_qkv, grad_w_out.reshape(heads, dim, d_model),
                early[2], early[0], early[1], grad_w_up, grad_b_up, grad_w_down, early[3])

    act_spec = P("dp", "tp", None)
    vec_spec = P(None)
    group_vec = P("dp")
    in_specs = (act_spec, act_spec, vec_spec, vec_spec, P(None, None, "tp", None), P(None, "tp", None), P("tp", None, None), vec_spec, vec_spec, vec_spec, P(None, "tp"), P("tp"), P("tp", None), vec_spec)
    out_specs = (act_spec, act_spec, group_vec, group_vec, P("dp", None, "tp", None), P("dp", "tp", None), P(("dp", "tp"), None, None), group_vec, group_vec, group_vec, P("dp", "tp"), P(("dp", "tp")), P(("dp", "tp"), None), group_vec)
    return jax.shard_map(device_step, mesh=mesh, in_specs=in_specs, out_specs=out_specs, check_vma=False)
```
